512 devices in a mesh: row: 16 (over y, core), col: 32 (over z, x).
Axes of the slice: x: 4, y: 8, z: 8, core: 2. Of those that a mesh axis runs over, the one named last changes fastest.
Arguments:
- matrix: float32 [16384, 16384], P('row', 'col'), as said below
Outputs:
- hess_panel: float32 [16384, 8], P('row')
- reflectors: float32 [16384, 8], P('row')
- wy_products: float32 [16384, 8], P('row')
- wy_factor: float32 [8, 8], replicated
Inputs may be any that keep to these rules, and one draw needn't show every extreme that they name: Entries matrix[i+1, i] lie within 2.5 +- 6 / sqrt(16384); every other entry within +- 6 / sqrt(16384).
All inputs are finite; a program needn't handle non-finite values.
Results may differ from the reference program's by a relative error of at most 0.0003.
Values sent between devices are 32-bit elements; how exact they have to be, the bound alone decides.
A program may use at most 128 MiB of HBM per device.

```python
import math
import jax
import jax.numpy as jnp
from jax import lax

N = 16384
NB = 8


def draw_matrix(key, part):
    first = jax.random.fold_in(key, 11)
    base = jax.random.truncated_normal(first, -6.0, 6.0, (N, N), jnp.float32)
    return base / math.sqrt(N) + 2.5 * jnp.eye(N, k=-1, dtype=jnp.float32)


def setup_inputs(seed: int = 0) -> dict:
    key_of = jax.random.split(jax.random.key(seed), 2)
    matrix = draw_matrix(jax.random.fold_in(key_of[1], 71), 0)
    return {"matrix": matrix}


def reference(matrix):
    exact = lax.Precision.HIGHEST
    order = matrix.shape[0]
    row_ids = jnp.arange(order, dtype=jnp.int32)
    refl = jnp.zeros((order, NB), jnp.float32)
    wy_prod = jnp.zeros((order, NB), jnp.float32)
    factor = jnp.zeros((NB, NB), jnp.float32)
    columns = []
    for column in range(NB):
        current = matrix[:, column] - jnp.dot(wy_prod, refl[column], precision=exact)
        inner = jnp.dot(current, refl, precision=exact)
        current = current - jnp.dot(refl, jnp.dot(inner, factor, precision=exact), precision=exact)
        masked = jnp.where(row_ids > column, current, jnp.float32(0.0))
        leading = current[column + 1]
        length = jnp.sqrt(jnp.sum(masked * masked))
        orient = jnp.where(leading >= 0, jnp.float32(1.0), jnp.float32(-1.0))
        pivot_value = -orient * length
        vector = masked + jnp.where(row_ids == column + 1, orient * length, jnp.float32(0.0))
        vector = vector / jnp.sqrt(length * (length + jnp.abs(leading)))
        coupling = jnp.dot(vector, refl, precision=exact)
        image = jnp.dot(matrix, vector, precision=exact)
        new_y = image - jnp.dot(wy_prod, coupling, precision=exact)
        new_t = -jnp.dot(factor, coupling, precision=exact)
        factor = factor.at[:, column].set(new_t).at[column, column].set(jnp.float32(1.0))
        wy_prod = wy_prod.at[:, column].set(new_y)
        refl = refl.at[:, column].set(vector)
        columns.append(jnp.where(row_ids <= column, current, jnp.where(row_ids == column + 1, pivot_value, jnp.float32(0.0))))
    return (jnp.stack(columns, axis=1), refl, wy_prod, factor)
```

```python
import functools

import jax
import jax.numpy as jnp
from jax import lax
from jax.experimental import pallas as pl
from jax.experimental.pallas import tpu as pltpu
from jax.sharding import PartitionSpec as P

NB = 8
TILE = (8, 128)


def across(value, shift):
    return pltpu.roll(value, shift, 0)


def row_sums(tiles, row):
    half = []
    for i in range(4):
        keep = jnp.where(row < 4, tiles[i], tiles[i + 4])
        give = jnp.where(row < 4, tiles[i + 4], tiles[i])
        half.append(keep + across(give, 4))
    quarter = []
    for i in range(2):
        a, b = half[i], half[i + 2]
        quarter.append(jnp.where(row % 4 < 2, a + across(a, 6), b + across(b, 2)))
    a, b = quarter
    return jnp.where(row % 2 < 1, a + across(a, 7), b + across(b, 1))


def tree(values):
    values = list(values)
    while len(values) > 1:
        paired = [values[i] + values[i + 1] for i in range(0, len(values) - 1, 2)]
        if len(values) % 2:
            paired.append(values[-1])
        values = paired
    return values[0]


def inverse_root(value):
    root = lax.rsqrt(value)
    return root * (1.5 - 0.5 * value * root * root)


def kernel(
    R, C, a_ref, hess_ref, v_ref, y_ref, t_ref,
    abuf, at, colt, first, acol_out, acol, xin, xl, zin, zout, vy,
    uhead, qhead, inv_nu, tcols, hcols, signs,
    a_sem, x_sem, z_sem, vy_sem, acol_sem, send_sem,
):
    f32 = jnp.float32
    r, c = lax.axis_index("row"), lax.axis_index("col")
    half = c - 2 * r
    owner = jnp.logical_and(half >= 0, half <= 1)
    seg_row = c // 2
    seg_half = c % 2
    corner = jnp.logical_and(r == 0, c == 0)
    row = lax.broadcasted_iota(jnp.int32, TILE, 0)
    lane = lax.broadcasted_iota(jnp.int32, TILE, 1)
    lane1 = lane[0:1]
    chunks = a_ref.shape[0] // 128
    blocks = a_ref.shape[1] // 128

    def chunk_copy(m):
        rows = pl.ds(pl.multiple_of(m * 128, 128), 128)
        return pltpu.make_async_copy(a_ref.at[rows, :], abuf.at[rows, :], a_sem.at[m])

    for m in range(chunks):
        chunk_copy(m).start()

    barrier = pltpu.get_barrier_semaphore()

    def greet(to_row, to_col):
        pl.semaphore_signal(
            barrier, inc=1, device_id={"row": to_row, "col": to_col},
            device_id_type=pl.DeviceIdType.MESH,
        )

    @pl.when(jnp.logical_not(corner))
    def _():
        greet(seg_row, 0)

    @pl.when(jnp.logical_not(owner))
    def _():
        greet(seg_row, c)

    for h in range(2):
        @pl.when(half != h)
        def _():
            greet(r, 2 * r + h)

    @pl.when(owner)
    def _():
        def body(k, carry):
            greet(r, (c + 1 + k) % C)
            return carry
        lax.fori_loop(0, C - 1, body, 0)

    zero = jnp.zeros(TILE, f32)
    for i in range(NB + 1):
        xl[i] = zero
    for ref in (uhead, qhead, inv_nu, tcols, hcols):
        ref[...] = zero
    for i in range(2):
        for k in range(9):
            vy[i, 8 * k : 8 * k + 8, :] = zero
    signs[...] = jnp.where(lane == 0, f32(1.0), f32(0.0))

    def turn(m, carry):
        chunk_copy(m).wait()
        rows = pl.ds(pl.multiple_of(m * 128, 128), 128)
        for t in range(blocks):
            at[128 * t : 128 * t + 128, rows] = abuf[rows, 128 * t : 128 * t + 128].T
        return carry

    lax.fori_loop(0, chunks, turn, 0)

    @pl.when(c == 0)
    def _():
        for k in range(NB + 1):
            for m in range(chunks):
                colt[k, m : m + 1, :] = at[k : k + 1, 128 * m : 128 * m + 128]
        unit = jnp.where(jnp.logical_and(row == 4, lane == 0), f32(1.0), f32(0.0))
        lead = colt[0]
        first[0] = jnp.where(row < 4, lead, jnp.where(r == 0, unit, zero))
        first[1] = jnp.where(row < 4, across(lead, 4), zero)
        for k in range(NB):
            acol_out[0, k] = across(colt[k + 1], 4)
            acol_out[1, k] = colt[k + 1]

    expected = (
        jnp.where(c == 0, 2 * R, 0) - jnp.where(corner, 1, 0)
        + jnp.where(owner, R + C - 3, 0) + 2
    )
    pl.semaphore_wait(barrier, expected)

    def remote(src, dst, sent, landed, to_row, to_col):
        return pltpu.make_async_remote_copy(
            src_ref=src, dst_ref=dst, send_sem=sent, recv_sem=landed,
            device_id={"row": to_row, "col": to_col},
            device_id_type=pl.DeviceIdType.MESH,
        )

    def await_bytes(ref, sem):
        pltpu.make_async_copy(ref, ref, sem).wait()

    @pl.when(c == 0)
    def _():
        for h in range(2):
            def body(k, carry):
                to = (r + R // 2 + k) % R

                @pl.when(jnp.logical_or(to != r, 2 * r + h != 0))
                def _():
                    remote(
                        first.at[h], xin.at[0], send_sem.at[0], x_sem.at[0], to, 2 * r + h
                    ).start()
                return carry
            lax.fori_loop(0, R, body, 0)
        for h in range(2):
            @pl.when(2 * r + h != 0)
            def _():
                remote(
                    acol_out.at[h], acol, send_sem.at[1], acol_sem, r, 2 * r + h
                ).start()

    @pl.when(corner)
    def _():
        xin[0] = first[0]
        for k in range(NB):
            acol[k] = acol_out[0, k]

    def column(j, carry):
        @pl.when(jnp.logical_not(jnp.where(j == 0, corner, owner)))
        def _():
            await_bytes(xin.at[j], x_sem.at[j])

        x = xin[j]
        xl[j] = x
        swapped = across(x, 4)
        mine = jnp.where(row < 4, f32(0.0), swapped)

        acc = jnp.zeros((8, 128 * chunks), f32)
        for t in range(blocks):
            spread = jnp.broadcast_to(x[t : t + 1, :], (128, 128)).T
            for k in range(16):
                part = spread[8 * k : 8 * k + 8, :]
                at_row = 128 * t + 8 * k
                acc = acc + at[at_row : at_row + 8, :] * jnp.concatenate([part] * chunks, 1)
        z = row_sums([acc[:, 128 * m : 128 * m + 128] for m in range(chunks)], row)

        sums = row_sums([xl[i] * mine for i in range(NB)], row)
        inner = jnp.sum(sums, axis=1, keepdims=True)
        inner = jnp.sum(jnp.where(lane == row, inner, f32(0.0)), axis=0, keepdims=True)
        square = jnp.sum(mine * mine, axis=0, keepdims=True)
        square = jnp.sum(square, axis=1, keepdims=True)
        shares = inner + jnp.where(lane1 == NB, square, f32(0.0))
        b_top = jnp.where(c == 0, x[0:1], f32(0.0))
        q_top = jnp.where(c == 0, x[4:5], f32(0.0))
        extra = jnp.where(row == 4, shares, jnp.where(row == 5, b_top, q_top))
        extra = jnp.where(row == 7, f32(0.0), extra)
        zout[j, 0] = jnp.where(row < 4, z, extra)
        zout[j, 1] = jnp.where(row < 4, across(z, 4), extra)

        for h in range(2):
            @pl.when(half != h)
            def _():
                slot = (c - (2 * r + h) + C) % C - 1
                remote(
                    zout.at[j, h], zin.at[(C - 1) * j + slot],
                    send_sem.at[2], z_sem.at[j], r, 2 * r + h,
                ).start()

        @pl.when(owner)
        def _():
            base = (C - 1) * j
            await_bytes(zin.at[pl.ds(base, C - 1)], z_sem.at[j])
            total = tree([zin[base + k] for k in range(C - 1)] + [zout[j, half]])
            coef = [jnp.broadcast_to(total[4:5, i : i + 1], TILE) for i in range(NB)]
            norm2 = jnp.broadcast_to(total[4:5, NB : NB + 1], TILE)
            norm2 = norm2 - tree([v * v for v in coef])
            inv_norm = inverse_root(norm2)
            fresh = jnp.where(row < 4, total, swapped)
            fresh = fresh - tree([coef[i] * xl[i] for i in range(NB)])
            fresh = fresh * inv_norm
            xin[j + 1] = fresh

            @pl.when(j < NB - 1)
            def _():
                for k in range(R - 1):
                    away = R // 2 + (k // 2 if k % 2 == 0 else -(k + 1) // 2)
                    remote(
                        xin.at[j + 1], xin.at[j + 1], send_sem.at[3], x_sem.at[j + 1],
                        (r + away) % R, c,
                    ).start()

            @pl.when(jnp.logical_and(j == 0, jnp.logical_not(corner)))
            def _():
                await_bytes(acol, acol_sem)

            norm = norm2[0:1] * inv_norm[0:1]
            top_b, top_q = total[5:6], total[6:7]
            qhead[pl.ds(j, 1), :] = top_q
            top = top_b - tree([coef[i][0:1] * qhead[i : i + 1] for i in range(NB)])
            rest = top * inv_norm[0:1]
            solve = []
            for m in range(NB - 1):
                g = -jnp.broadcast_to(rest[:, m + 1 : m + 2], (1, 128)) * inv_nu[m : m + 1]
                rest = rest + g * uhead[m : m + 1]
                solve.append(g)
            pivot = jnp.sum(jnp.where(lane1 == j + 1, rest, f32(0.0)), axis=1, keepdims=True)
            sign_at = jnp.where(lane1 == j, signs[0:1], f32(0.0))
            sign = jnp.broadcast_to(jnp.sum(sign_at, axis=1, keepdims=True), (1, 128))
            pivot = sign * pivot
            orient = jnp.where(pivot >= 0, f32(1.0), f32(-1.0))
            grown = 1.0 + jnp.abs(pivot)
            inv_root = inverse_root(grown)
            inv_pivot = orient * inv_root
            next_sign = -sign * orient
            unit = jnp.where(lane1 == j + 1, f32(1.0), f32(0.0))
            new_head = (sign * rest + orient * unit) * inv_root
            new_head = jnp.where(lane1 > j, new_head, f32(0.0))

            weights = jnp.sum(
                jnp.where(lane == j + 1, uhead[...], f32(0.0)), axis=1, keepdims=True
            )
            weights = jnp.broadcast_to(weights, TILE)
            tcol = jnp.where(lane1 == j, orient * grown * inv_root, f32(0.0))
            for m in range(NB - 1):
                tcol = tcol + jnp.where(lane1 == m, next_sign * solve[m], f32(0.0))
            used = jnp.sum(weights * tcols[...], axis=0, keepdims=True)
            tcols[pl.ds(j, 1), :] = (tcol - used) * inv_pivot

            hcol = jnp.where(lane1 <= j, sign * signs[0:1] * total[4:5], f32(0.0))
            hcol = hcol + jnp.where(lane1 == j + 1, sign * next_sign * norm, f32(0.0))
            hcols[pl.ds(j, 1), :] = hcol

            turned = across(fresh, 4)
            out = jnp.where(row < 4, turned, acol[j] - next_sign * turned)
            for m in range(NB - 1):
                out = out + jnp.where(row < 4, solve[m], -weights[m : m + 1]) * (
                    vy[half, 8 * m : 8 * m + 8, :]
                )
            out = out * jnp.where(row < 4, sign * inv_root, inv_pivot)
            index = 512 * c + 128 * row + lane
            out = out + jnp.where(
                jnp.logical_and(row < 4, index == j + 1), inv_pivot, f32(0.0)
            )
            out = jnp.where(jnp.logical_and(row < 4, index <= j), f32(0.0), out)
            vy[half, pl.ds(pl.multiple_of(8 * j, 8), 8), :] = out

            uhead[pl.ds(j, 1), :] = new_head
            inv_nu[pl.ds(j, 1), :] = jnp.broadcast_to(inv_pivot, (1, 128))
            signs[...] = jnp.where(lane == j + 1, next_sign, signs[...])

            @pl.when(j < NB - 1)
            def _():
                def body(k, carry):
                    part = vy.at[half, pl.ds(pl.multiple_of(8 * j, 8), 8), :]
                    remote(
                        part, part, send_sem.at[4], vy_sem.at[half], r, (c + 1 + k) % C
                    ).start()
                    return carry
                lax.fori_loop(0, C - 1, body, 0)

            @pl.when(j == NB - 1)
            def _():
                vy[half, 64:72, :] = jnp.where(half == 0, tcols[...], hcols[...])

                def body(k, carry):
                    to = (c + C // 2 + k) % C

                    @pl.when(to != c)
                    def _():
                        part = vy.at[half, 56:72, :]
                        remote(
                            part, part, send_sem.at[5], vy_sem.at[half], r, to
                        ).start()
                    return carry
                lax.fori_loop(0, C, body, 0)

        return carry

    lax.fori_loop(0, NB, column, 0)

    for h in range(2):
        @pl.when(half != h)
        def _():
            await_bytes(vy.at[h], vy_sem.at[h])

    for h in range(2):
        for t in range(4):
            at_lane = 128 * (4 * h + t)
            v_ref[:, at_lane : at_lane + 128] = vy[h, pl.ds(t, 8, stride=8), :]
            y_ref[:, at_lane : at_lane + 128] = vy[h, pl.ds(t + 4, 8, stride=8), :]
    hess_ref[...] = jnp.zeros(hess_ref.shape, f32)
    hess_ref[:, 0:128] = jnp.where(r == 0, vy[1, 64:72, :], f32(0.0))
    t_ref[...] = vy[0, 64:72, 0:NB]

    def await_tiles(count, sem):
        await_bytes(zin.at[pl.ds(0, count)], sem)

    @pl.when(c == 0)
    def _():
        @pl.when(corner)
        def _():
            await_tiles(2 * R - 1, send_sem.at[0])
            await_bytes(acol, send_sem.at[1])

        @pl.when(jnp.logical_not(corner))
        def _():
            await_tiles(2 * R, send_sem.at[0])
            await_bytes(acol_out, send_sem.at[1])

    @pl.when(jnp.logical_not(owner))
    def _():
        await_tiles(2 * NB, send_sem.at[2])

    @pl.when(owner)
    def _():
        await_tiles(NB, send_sem.at[2])
        await_tiles((NB - 1) * (R - 1), send_sem.at[3])
        await_tiles((NB - 1) * (C - 1), send_sem.at[4])
        await_tiles(2 * (C - 1), send_sem.at[5])


def shards(R, C, matrix):
    rows, cols = matrix.shape
    f32 = jnp.float32
    wide = jax.ShapeDtypeStruct((NB, rows), f32)
    vmem = pl.BlockSpec(memory_space=pltpu.VMEM)
    scratch = [
        pltpu.VMEM((rows, cols), f32),
        pltpu.VMEM((cols, rows), f32),
        pltpu.VMEM((NB + 1, 8, 128), f32),
        pltpu.VMEM((2, 8, 128), f32),
        pltpu.VMEM((2, NB, 8, 128), f32),
        pltpu.VMEM((NB, 8, 128), f32),
        pltpu.VMEM((NB + 1, 8, 128), f32),
        pltpu.VMEM((NB + 1, 8, 128), f32),
        pltpu.VMEM((NB * (C - 1), 8, 128), f32),
        pltpu.VMEM((NB, 2, 8, 128), f32),
        pltpu.VMEM((2, 72, 128), f32),
    ]
    scratch += [pltpu.VMEM((8, 128), f32)] * 6
    scratch += [
        pltpu.SemaphoreType.DMA((rows // 128,)),
        pltpu.SemaphoreType.DMA((NB,)),
        pltpu.SemaphoreType.DMA((NB,)),
        pltpu.SemaphoreType.DMA((2,)),
        pltpu.SemaphoreType.DMA,
        pltpu.SemaphoreType.DMA((6,)),
    ]
    hess, refl, prod, factor = pl.pallas_call(
        functools.partial(kernel, R, C),
        out_shape=(wide, wide, wide, jax.ShapeDtypeStruct((NB, NB), f32)),
        in_specs=[pl.BlockSpec(memory_space=pl.ANY)],
        out_specs=(vmem,) * 4,
        scratch_shapes=scratch,
        compiler_params=pltpu.CompilerParams(collective_id=0, has_side_effects=True),
        name="panel",
    )(matrix)
    return hess.T, refl.T, prod.T, factor.T


def solution(mesh):
    R, C = mesh.shape["row"], mesh.shape["col"]
    return jax.shard_map(
        functools.partial(shards, R, C),
        mesh=mesh,
        in_specs=(P("row", "col"),),
        out_specs=(P("row", None), P("row", None), P("row", None), P()),
        check_vma=False,
    )
```
